16 devices in a mesh: dp: 1, sp: 16 (over x, y, z, core).
Axes of the slice: x: 2, y: 2, z: 2, core: 2. Of those that a mesh axis runs over, the one named last changes fastest.
Arguments:
- q: bfloat16 [32, 96, 192], P('dp')
- k: bfloat16 [32, 8192, 8, 192], P('dp', 'sp')
- v: bfloat16 [32, 8192, 8, 192], P('dp', 'sp')
Outputs:
- q: bfloat16 [32, 96, 192], P('dp')
All inputs are finite; a program needn't handle non-finite values.
Results may differ from the reference program's by a relative error of at most 0.012.
Values are sent between devices in bfloat16 or wider.
A program may use at most 2 GiB of HBM per device.

```python
import jax
import jax.numpy as jnp

BATCH = 32
CACHE = 8192
HEADS = 96
KV_HEADS = 8
HEAD = 192


def setup_inputs(seed: int = 0, part: int = 0) -> dict:
    kq, kk, kv = (jax.random.fold_in(k, part) for k in jax.random.split(jax.random.key(seed), 3))
    return {
        "q": (3 * jax.random.normal(kq, (BATCH, HEADS, HEAD), jnp.float32)).astype(jnp.bfloat16),
        "k": jax.random.normal(kk, (BATCH, CACHE, KV_HEADS, HEAD), jnp.float32).astype(jnp.bfloat16),
        "v": jax.random.normal(kv, (BATCH, CACHE, KV_HEADS, HEAD), jnp.float32).astype(jnp.bfloat16),
    }


def einsum(form, a, b):
    return jnp.einsum(form, a.astype(jnp.float32), b.astype(jnp.float32))


def reference(q, k, v):
    grouped = q.reshape(BATCH, KV_HEADS, -1, HEAD)
    scores = einsum("bgsd,bugd->bgsu", grouped, k) * HEAD**-0.5
    weights = jax.nn.softmax(scores, -1).astype(jnp.bfloat16)
    return einsum("bgsu,bugd->bgsd", weights, v).astype(jnp.bfloat16).reshape(BATCH, HEADS, HEAD)
```

```python
import functools
import math

import jax
import jax.numpy as jnp
from jax import lax
from jax.experimental import pallas as pl
from jax.experimental.pallas import tpu as pltpu
from jax.sharding import PartitionSpec as P

MESH = pl.DeviceIdType.MESH
RING = 4


def wait_for(ref, sem):
    pltpu.make_async_copy(ref, ref, sem).wait()


def kernel(
    scale,
    q_hbm,
    k_hbm,
    v_hbm,
    out,
    q,
    kbuf,
    vbuf,
    scores,
    highs,
    mine,
    mine_st,
    other,
    other_st,
    part,
    part_st,
    sums,
    stats,
    q_sem,
    k_sem,
    v_sem,
    d_send,
    d_recv,
    dst_send,
    dst_recv,
    s_send,
    s_recv,
    st_send,
    st_recv,
    rel_send,
    rel_recv,
):
    pairs = k_hbm.shape[0] // 2
    me = lax.axis_index("sp")
    core = me % 2
    partner = me + 1 - 2 * core
    bits = [me // 8, (me // 4) % 2, (me // 2) % 2]
    peers = [me + n - 2 * n * bit for n, bit in zip((8, 4, 2), bits)]
    lane = lax.broadcasted_iota(jnp.int32, (8, 128), 1)
    row = lax.broadcasted_iota(jnp.int32, (8, 128), 0)
    spot = [lane == row + 8 * k for k in range(12)]
    row_low = lax.broadcasted_iota(jnp.int32, (8, 512), 0) < 4
    lane_low = lane < 64
    power = scale * math.log2(math.e)

    def seq(p, j):
        return 2 * p + (1 - core) + j * (2 * core - 1)

    def k_copy(p, j):
        slot = 2 * (p % RING) + j
        return pltpu.make_async_copy(k_hbm.at[seq(p, j)], kbuf.at[slot], k_sem.at[slot])

    def v_copy(p, j):
        slot = 2 * (p % RING) + j
        return pltpu.make_async_copy(v_hbm.at[seq(p, j)], vbuf.at[slot], v_sem.at[slot])

    def send(src, dst, ssem, rsem, to):
        pltpu.make_async_remote_copy(
            src_ref=src, dst_ref=dst, send_sem=ssem, recv_sem=rsem, device_id={"sp": to}, device_id_type=MESH
        ).start()

    def factors(a, b, last):
        high = jnp.maximum(a[:1], b[:1])
        fa, fb = jnp.exp2((a[:1] - high) * power), jnp.exp2((b[:1] - high) * power)
        total = fa * a[1:] + fb * b[1:]
        if last:
            fa, fb = fa / total, fb / total

        def columns(f):
            f = jnp.broadcast_to(f, (8, 128))
            c = [jnp.sum(jnp.where(here, f, 0.0), 1, keepdims=True) for here in spot]
            return c + [jnp.where(lane_low, c[k], c[k + 6]) for k in range(6)]

        return columns(fa), columns(fb), jnp.concatenate([high, total], 0)

    def added(a, b, fa, fb):
        return [
            a[8 * k : 8 * k + 8].astype(jnp.float32) * fa[k] + b[8 * k : 8 * k + 8].astype(jnp.float32) * fb[k]
            for k in range(18)
        ]

    def slot_of(p):
        if isinstance(p, int):
            return p if 0 <= p < pairs else pairs
        return jnp.where(p >= 0, p, pairs)

    def add(p, s):
        n = slot_of(p)
        if s == 0:
            a, b, sa, sb = mine[n % 4], part[n], mine_st[n % 4], part_st[n]
        else:
            a, b, sa, sb = sums[s - 1, n, 0], sums[s - 1, n, 1], stats[s - 1, n, 0], stats[s - 1, n, 1]
        fa, fb, st = factors(sa, sb, s == 3)
        tiles = added(a, b, fa, fb)
        if s < 3:
            sums[s, n, bits[s]] = jnp.concatenate(tiles, 0).astype(jnp.bfloat16)
            stats[s, n, bits[s]] = st
            return
        b = seq(max(p, 0) if isinstance(p, int) else jnp.where(p >= 0, p, 0), 1)
        out[b, :, :128] = jnp.concatenate(tiles[:12], 0).astype(out.dtype)
        rest = jnp.concatenate(tiles[12:], 0)
        out[b, :48, 128:] = rest[:, :64].astype(out.dtype)
        out[b, 48:, 128:] = rest[:, 64:].astype(out.dtype)

    def start(p, s):
        if s == 0:
            send(other.at[p], part.at[p], d_send.at[p], d_recv.at[p], partner)
            send(other_st.at[p], part_st.at[p], dst_send.at[p], dst_recv.at[p], partner)
        elif s < 4:
            s = s - 1
            at = (s, p, bits[s])
            send(sums.at[at], sums.at[at], s_send.at[s, p], s_recv.at[s, p], peers[s])
            send(stats.at[at], stats.at[at], st_send.at[s, p], st_recv.at[s, p], peers[s])
        else:
            b = seq(p, 1)
            send(out.at[b], out.at[b], rel_send.at[p], rel_recv.at[p], partner)

    def arrive(p, s):
        if s == 0:
            wait_for(part.at[p], d_recv.at[p])
            wait_for(part_st.at[p], dst_recv.at[p])
        else:
            wait_for(part.at[p], s_recv.at[s - 1, p])
            wait_for(part_st.at[p], st_recv.at[s - 1, p])

    SEND = (2, 4, 7, 10, 13)
    ADD = (3, 6, 9, 12)

    def keys(p):
        for j in range(2):
            b = seq(p, j)
            slot = 2 * (p % RING) + j
            srow = 2 * (p % 2) + j
            acc = jnp.zeros((8, 128), jnp.float32)
            for h in range(4):
                low = jnp.dot(q[b, 24 * h : 24 * h + 16], kbuf[slot, 2 * h], preferred_element_type=jnp.float32)
                top = jnp.dot(q[b, 24 * h + 8 : 24 * h + 24], kbuf[slot, 2 * h + 1], preferred_element_type=jnp.float32)
                tiles = (low[:8], jnp.where(row_low, low[8:], top[:8]), top[8:])
                for t, tile in enumerate(tiles):
                    k = 3 * h + t
                    scores[srow, 8 * k : 8 * k + 8] = tile
                    high = jnp.max(tile, 1, keepdims=True)
                    highs[srow, 8 * k : 8 * k + 8] = jnp.broadcast_to(high, (8, 128))
                    acc = jnp.where(spot[k], high, acc)
            st = jnp.sum(acc, 0, keepdims=True)
            if j == 0:
                other_st[p, :1] = st
            else:
                mine_st[p % 4, :1] = st

    def values(p):
        for j in range(2):
            slot = 2 * (p % RING) + j
            srow = 2 * (p % 2) + j
            acc = jnp.zeros((8, 128), jnp.float32)
            rest = []
            for h in range(4):
                tiles = []
                for t in range(3):
                    k = 3 * h + t
                    top = highs[srow, 8 * k : 8 * k + 8, :1]
                    tile = jnp.exp2((scores[srow, 8 * k : 8 * k + 8] - top) * power)
                    acc = jnp.where(spot[k], jnp.sum(tile, 1, keepdims=True), acc)
                    tiles.append(tile)
                first = jnp.concatenate([tiles[0], jnp.where(row_low, tiles[1], 0.0)], 0).astype(jnp.bfloat16)
                second = jnp.concatenate([jnp.where(row_low, 0.0, tiles[1]), tiles[2]], 0).astype(jnp.bfloat16)
                dims = (((1,), (1,)), ((), ()))
                a = lax.dot_general(first, vbuf[slot, 2 * h], dims, preferred_element_type=jnp.float32)
                z = lax.dot_general(second, vbuf[slot, 2 * h + 1], dims, preferred_element_type=jnp.float32)
                seen = jnp.concatenate([a[:8], a[8:] + z[:8], z[8:]], 0)
                rest.append(seen[:, 128:])
                if j == 0:
                    other[p, 24 * h : 24 * h + 24] = seen[:, :128].astype(jnp.bfloat16)
                else:
                    mine[p % 4, 24 * h : 24 * h + 24] = seen[:, :128]
            rest = jnp.concatenate([jnp.concatenate(rest[:2], 0), jnp.concatenate(rest[2:], 0)], 1)
            st = jnp.sum(acc, 0, keepdims=True)
            if j == 0:
                other[p, 96:] = rest.astype(jnp.bfloat16)
                other_st[p, 1:] = st
            else:
                mine[p % 4, 96:] = rest
                mine_st[p % 4, 1:] = st

    q_copy = pltpu.make_async_copy(q_hbm, q, q_sem)
    k_copy(0, 0).start()
    q_copy.start()
    k_copy(0, 1).start()
    for copy, p in ((k_copy, 1), (v_copy, 0), (k_copy, 2), (v_copy, 1)):
        for j in range(2):
            copy(p, j).start()
    barrier = pltpu.get_barrier_semaphore()
    for to in (partner, *peers):
        pl.semaphore_signal(barrier, inc=1, device_id={"sp": to}, device_id_type=MESH)
    q_copy.wait()
    pl.semaphore_wait(barrier, 4)

    def when(condition, what):
        if isinstance(condition, bool):
            if condition:
                what()
        else:
            pl.when(condition)(what)

    def body(u):
        first, last = isinstance(u, int) and u == 0, isinstance(u, int) and u == pairs
        for j in range(2):
            if not last:
                k_copy(u, j).wait()
            if not first:
                v_copy(u - 1, j).wait()

        def more_keys():
            for j in range(2):
                k_copy(u + 3, j).start()

        def more_values():
            for j in range(2):
                v_copy(u + 2, j).start()

        when(u + 3 < pairs, more_keys)
        when(u + 2 < pairs, more_values)
        for s, lag in enumerate(ADD):
            when(u - lag >= 0, lambda: arrive(u - lag, s))
        for s, lag in enumerate(SEND):
            when(u - lag >= 0, lambda: start(u - lag, s))
        if not last:
            keys(u)
        if not first:
            values(u - 1)
        if not first:
            for s, lag in enumerate(ADD):
                add(u - lag, s)

    body(0)
    lax.fori_loop(1, pairs, lambda u, c: (body(u), c)[1], 0)
    body(pairs)

    todo = []
    for p in range(pairs):
        sent = [s for s in range(5) if p + SEND[s] <= pairs]
        done = [s for s in range(4) if p + ADD[s] <= pairs]
        time = 0.0
        if len(sent) == len(done) < 5:
            todo.append((time, p, len(done), False))
        for s in range(len(done), 4):
            time = max(time + (1.2 if s == 0 else 2.7), 0.0) if s >= len(sent) else (p + SEND[s] - pairs) * 1.5 + 2.0
            time = max(time, 0.0)
            todo.append((time, p, s, True))
    for _, p, s, arrives in sorted(todo):
        if arrives:
            arrive(p, s)
            add(p, s)
            start(p, s + 1)
        else:
            start(p, s)
    for p in range(pairs):
        wait_for(out.at[0], rel_recv.at[p])
        wait_for(out.at[0], rel_send.at[p])
        wait_for(part.at[p], d_send.at[p])
        wait_for(part_st.at[p], dst_send.at[p])
        for s in range(3):
            wait_for(part.at[p], s_send.at[s, p])
            wait_for(part_st.at[p], st_send.at[s, p])


def solution(mesh):
    def step(q, k, v):
        seqs, heads, head = q.shape
        tokens, kv = k.shape[1:3]
        pairs, packed = seqs // 2, heads + heads // 2
        kt = jnp.transpose(k, (0, 2, 3, 1))
        vt = jnp.transpose(v, (0, 2, 3, 1))
        f32, bf16 = jnp.float32, jnp.bfloat16
        vm, dma = pltpu.VMEM, pltpu.SemaphoreType.DMA
        anywhere = pl.BlockSpec(memory_space=pl.ANY)
        return pl.pallas_call(
            functools.partial(kernel, head**-0.5),
            out_shape=jax.ShapeDtypeStruct(q.shape, q.dtype),
            in_specs=[anywhere] * 3,
            out_specs=pl.BlockSpec(memory_space=pltpu.VMEM),
            scratch_shapes=[
                vm((seqs, heads, head), bf16),
                vm((2 * RING, kv, head, tokens), bf16),
                vm((2 * RING, kv, head, tokens), bf16),
                vm((4, heads, tokens), f32),
                vm((4, heads, 128), f32),
                vm((4, packed, 128), f32),
                vm((4, 2, 128), f32),
                vm((pairs, packed, 128), bf16),
                vm((pairs, 2, 128), f32),
                vm((pairs + 1, packed, 128), bf16),
                vm((pairs + 1, 2, 128), f32),
                vm((3, pairs + 1, 2, packed, 128), bf16),
                vm((3, pairs + 1, 2, 2, 128), f32),
                dma(()),
                dma((2 * RING,)),
                dma((2 * RING,)),
                *[dma((pairs,))] * 4,
                *[dma((3, pairs))] * 4,
                *[dma((pairs,))] * 2,
            ],
            compiler_params=pltpu.CompilerParams(
                collective_id=0, has_side_effects=True, vmem_limit_bytes=60 << 20
            ),
            name="decode",
        )(q, kt, vt)

    return jax.shard_map(
        step,
        mesh=mesh,
        in_specs=(P("dp", None, None), P("dp", "sp", None, None), P("dp", "sp", None, None)),
        out_specs=P("dp", None, None),
        check_vma=False,
    )
```

```python
import functools
import math

import jax
import jax.numpy as jnp
from jax import lax
from jax.experimental import pallas as pl
from jax.experimental.pallas import tpu as pltpu
from jax.sharding import PartitionSpec as P

MESH = pl.DeviceIdType.MESH
RING = 4


def wait_for(ref, sem):
    pltpu.make_async_copy(ref, ref, sem).wait()


def kernel(
    scale,
    q_hbm,
    k_hbm,
    v_hbm,
    out,
    q,
    kbuf,
    vbuf,
    scores,
    highs,
    mine,
    mine_st,
    other,
    other_st,
    part,
    part_st,
    sums,
    stats,
    q_sem,
    k_sem,
    v_sem,
    d_send,
    d_recv,
    dst_send,
    dst_recv,
    s_send,
    s_recv,
    st_send,
    st_recv,
    rel_send,
    rel_recv,
):
    pairs = k_hbm.shape[0] // 2
    me = lax.axis_index("sp")
    core = me % 2
    partner = me + 1 - 2 * core
    bits = [me // 8, (me // 4) % 2, (me // 2) % 2]
    peers = [me + n - 2 * n * bit for n, bit in zip((8, 4, 2), bits)]
    lane = lax.broadcasted_iota(jnp.int32, (8, 128), 1)
    row = lax.broadcasted_iota(jnp.int32, (8, 128), 0)
    spot = [lane == row + 8 * k for k in range(12)]
    row_low = lax.broadcasted_iota(jnp.int32, (8, 512), 0) < 4
    lane_low = lane < 64
    power = scale * math.log2(math.e)

    def seq(p, j):
        return 2 * p + (1 - core) + j * (2 * core - 1)

    def k_copy(p, j):
        slot = 2 * (p % RING) + j
        return pltpu.make_async_copy(k_hbm.at[seq(p, j)], kbuf.at[slot], k_sem.at[slot])

    def v_copy(p, j):
        slot = 2 * (p % RING) + j
        return pltpu.make_async_copy(v_hbm.at[seq(p, j)], vbuf.at[slot], v_sem.at[slot])

    def send(src, dst, ssem, rsem, to):
        pltpu.make_async_remote_copy(
            src_ref=src, dst_ref=dst, send_sem=ssem, recv_sem=rsem, device_id={"sp": to}, device_id_type=MESH
        ).start()

    def factors(a, b, last):
        high = jnp.maximum(a[:1], b[:1])
        fa, fb = jnp.exp2((a[:1] - high) * power), jnp.exp2((b[:1] - high) * power)
        total = fa * a[1:] + fb * b[1:]
        if last:
            fa, fb = fa / total, fb / total

        def columns(f):
            f = jnp.broadcast_to(f, (8, 128))
            c = [jnp.sum(jnp.where(here, f, 0.0), 1, keepdims=True) for here in spot]
            return c + [jnp.where(lane_low, c[k], c[k + 6]) for k in range(6)]

        return columns(fa), columns(fb), jnp.concatenate([high, total], 0)

    def added(a, b, fa, fb):
        return [
            a[8 * k : 8 * k + 8].astype(jnp.float32) * fa[k] + b[8 * k : 8 * k + 8].astype(jnp.float32) * fb[k]
            for k in range(18)
        ]

    def slot_of(p):
        if isinstance(p, int):
            return p if 0 <= p < pairs else pairs
        return jnp.where(p >= 0, p, pairs)

    def add(p, s):
        n = slot_of(p)
        if s == 0:
            a, b, sa, sb = mine[n % 4], part[n], mine_st[n % 4], part_st[n]
        else:
            a, b, sa, sb = sums[s - 1, n, 0], sums[s - 1, n, 1], stats[s - 1, n, 0], stats[s - 1, n, 1]
        fa, fb, st = factors(sa, sb, s == 3)
        tiles = added(a, b, fa, fb)
        if s < 3:
            sums[s, n, bits[s]] = jnp.concatenate(tiles, 0).astype(jnp.bfloat16)
            stats[s, n, bits[s]] = st
            return
        b = seq(max(p, 0) if isinstance(p, int) else jnp.where(p >= 0, p, 0), 1)
        out[b, :, :128] = jnp.concatenate(tiles[:12], 0).astype(out.dtype)
        rest = jnp.concatenate(tiles[12:], 0)
        out[b, :48, 128:] = rest[:, :64].astype(out.dtype)
        out[b, 48:, 128:] = rest[:, 64:].astype(out.dtype)

    def start(p, s):
        if s == 0:
            send(other.at[p], part.at[p], d_send.at[p], d_recv.at[p], partner)
            send(other_st.at[p], part_st.at[p], dst_send.at[p], dst_recv.at[p], partner)
        elif s < 4:
            s = s - 1
            at = (s, p, bits[s])
            send(sums.at[at], sums.at[at], s_send.at[s, p], s_recv.at[s, p], peers[s])
            send(stats.at[at], stats.at[at], st_send.at[s, p], st_recv.at[s, p], peers[s])
        else:
            b = seq(p, 1)
            send(out.at[b], out.at[b], rel_send.at[p], rel_recv.at[p], partner)

    def arrive(p, s):
        if s == 0:
            wait_for(part.at[p], d_recv.at[p])
            wait_for(part_st.at[p], dst_recv.at[p])
        else:
            wait_for(part.at[p], s_recv.at[s - 1, p])
            wait_for(part_st.at[p], st_recv.at[s - 1, p])

    SEND = (2, 4, 7, 10, 13)
    ADD = (3, 6, 9, 12)

    def keys(p):
        for j in range(2):
            b = seq(p, j)
            slot = 2 * (p % RING) + j
            srow = 2 * (p % 2) + j
            acc = jnp.zeros((8, 128), jnp.float32)
            for h in range(4):
                low = jnp.dot(q[b, 24 * h : 24 * h + 16], kbuf[slot, 2 * h], preferred_element_type=jnp.float32)
                top = jnp.dot(q[b, 24 * h + 8 : 24 * h + 24], kbuf[slot, 2 * h + 1], preferred_element_type=jnp.float32)
                tiles = (low[:8], jnp.where(row_low, low[8:], top[:8]), top[8:])
                for t, tile in enumerate(tiles):
                    k = 3 * h + t
                    scores[srow, 8 * k : 8 * k + 8] = tile
                    high = jnp.max(tile, 1, keepdims=True)
                    highs[srow, 8 * k : 8 * k + 8] = jnp.broadcast_to(high, (8, 128))
                    acc = jnp.where(spot[k], high, acc)
            st = jnp.sum(acc, 0, keepdims=True)
            if j == 0:
                other_st[p, :1] = st
            else:
                mine_st[p % 4, :1] = st

    def values(p):
        for j in range(2):
            slot = 2 * (p % RING) + j
            srow = 2 * (p % 2) + j
            acc = jnp.zeros((8, 128), jnp.float32)
            rest = []
            for h in range(4):
                tiles = []
                for t in range(3):
                    k = 3 * h + t
                    top = highs[srow, 8 * k : 8 * k + 8, :1]
                    tile = jnp.exp2((scores[srow, 8 * k : 8 * k + 8] - top) * power)
                    acc = jnp.where(spot[k], jnp.sum(tile, 1, keepdims=True), acc)
                    tiles.append(tile)
                first = jnp.concatenate([tiles[0], jnp.where(row_low, tiles[1], 0.0)], 0).astype(jnp.bfloat16)
                second = jnp.concatenate([jnp.where(row_low, 0.0, tiles[1]), tiles[2]], 0).astype(jnp.bfloat16)
                dims = (((1,), (1,)), ((), ()))
                a = lax.dot_general(first, vbuf[slot, 2 * h], dims, preferred_element_type=jnp.float32)
                z = lax.dot_general(second, vbuf[slot, 2 * h + 1], dims, preferred_element_type=jnp.float32)
                seen = jnp.concatenate([a[:8], a[8:] + z[:8], z[8:]], 0)
                rest.append(seen[:, 128:])
                if j == 0:
                    other[p, 24 * h : 24 * h + 24] = seen[:, :128].astype(jnp.bfloat16)
                else:
                    mine[p % 4, 24 * h : 24 * h + 24] = seen[:, :128]
            rest = jnp.concatenate([jnp.concatenate(rest[:2], 0), jnp.concatenate(rest[2:], 0)], 1)
            st = jnp.sum(acc, 0, keepdims=True)
            if j == 0:
                other[p, 96:] = rest.astype(jnp.bfloat16)
                other_st[p, 1:] = st
            else:
                mine[p % 4, 96:] = rest
                mine_st[p % 4, 1:] = st

    q_copy = pltpu.make_async_copy(q_hbm, q, q_sem)
    k_copy(0, 0).start()
    q_copy.start()
    k_copy(0, 1).start()
    for copy, p in ((k_copy, 1), (v_copy, 0), (k_copy, 2), (v_copy, 1)):
        for j in range(2):
            copy(p, j).start()
    barrier = pltpu.get_barrier_semaphore()
    for to in (partner, *peers):
        pl.semaphore_signal(barrier, inc=1, device_id={"sp": to}, device_id_type=MESH)
    q_copy.wait()
    pl.semaphore_wait(barrier, 4)

    def when(condition, what):
        if isinstance(condition, bool):
            if condition:
                what()
        else:
            pl.when(condition)(what)

    def body(u):
        first, last = isinstance(u, int) and u == 0, isinstance(u, int) and u == pairs
        for s, lag in enumerate(SEND):
            when(u - lag >= 0, lambda: start(u - lag, s))
        for j in range(2):
            if not last:
                k_copy(u, j).wait()
            if not first:
                v_copy(u - 1, j).wait()

        def more_keys():
            for j in range(2):
                k_copy(u + 3, j).start()

        def more_values():
            for j in range(2):
                v_copy(u + 2, j).start()

        when(u + 3 < pairs, more_keys)
        when(u + 2 < pairs, more_values)
        for s, lag in enumerate(ADD):
            when(u - lag >= 0, lambda: arrive(u - lag, s))
        if not last:
            keys(u)
        if not first:
            values(u - 1)
        if not first:
            for s, lag in enumerate(ADD):
                add(u - lag, s)

    body(0)
    lax.fori_loop(1, pairs, lambda u, c: (body(u), c)[1], 0)
    body(pairs)

    todo = []
    for p in range(pairs):
        sent = [s for s in range(5) if p + SEND[s] <= pairs]
        done = [s for s in range(4) if p + ADD[s] <= pairs]
        time = 0.0
        if len(sent) == len(done) < 5:
            todo.append((time, p, len(done), False))
        for s in range(len(done), 4):
            time = max(time + (1.2 if s == 0 else 2.7), 0.0) if s >= len(sent) else (p + SEND[s] - pairs) * 1.5 + 2.0
            time = max(time, 0.0)
            todo.append((time, p, s, True))
    for _, p, s, arrives in sorted(todo):
        if arrives:
            arrive(p, s)
            add(p, s)
            start(p, s + 1)
        else:
            start(p, s)
    for p in range(pairs):
        wait_for(out.at[0], rel_recv.at[p])
        wait_for(out.at[0], rel_send.at[p])
        wait_for(part.at[p], d_send.at[p])
        wait_for(part_st.at[p], dst_send.at[p])
        for s in range(3):
            wait_for(part.at[p], s_send.at[s, p])
            wait_for(part_st.at[p], st_send.at[s, p])


def solution(mesh):
    def step(q, k, v):
        seqs, heads, head = q.shape
        tokens, kv = k.shape[1:3]
        pairs, packed = seqs // 2, heads + heads // 2
        kt = jnp.transpose(k, (0, 2, 3, 1))
        vt = jnp.transpose(v, (0, 2, 3, 1))
        f32, bf16 = jnp.float32, jnp.bfloat16
        vm, dma = pltpu.VMEM, pltpu.SemaphoreType.DMA
        anywhere = pl.BlockSpec(memory_space=pl.ANY)
        return pl.pallas_call(
            functools.partial(kernel, head**-0.5),
            out_shape=pltpu.VMEM(q.shape, q.dtype),
            in_specs=[anywhere] * 3,
            out_specs=pl.BlockSpec(memory_space=pltpu.VMEM),
            scratch_shapes=[
                vm((seqs, heads, head), bf16),
                vm((2 * RING, kv, head, tokens), bf16),
                vm((2 * RING, kv, head, tokens), bf16),
                vm((4, heads, tokens), f32),
                vm((4, heads, 128), f32),
                vm((4, packed, 128), f32),
                vm((4, 2, 128), f32),
                vm((pairs, packed, 128), bf16),
                vm((pairs, 2, 128), f32),
                vm((pairs + 1, packed, 128), bf16),
                vm((pairs + 1, 2, 128), f32),
                vm((3, pairs + 1, 2, packed, 128), bf16),
                vm((3, pairs + 1, 2, 2, 128), f32),
                dma(()),
                dma((2 * RING,)),
                dma((2 * RING,)),
                *[dma((pairs,))] * 4,
                *[dma((3, pairs))] * 4,
                *[dma((pairs,))] * 2,
            ],
            compiler_params=pltpu.CompilerParams(
                collective_id=0, has_side_effects=True, vmem_limit_bytes=56 << 20
            ),
            name="decode",
        )(q, kt, vt)

    return jax.shard_map(
        step,
        mesh=mesh,
        in_specs=(P("dp", None, None), P("dp", "sp", None, None), P("dp", "sp", None, None)),
        out_specs=P("dp", None, None),
        check_vma=False,
    )
```
